32 devices in a mesh: graph: 8 (over y, x, core), rep: 4 (over z).
Axes of the slice: x: 2, y: 2, z: 4, core: 2. Of those that a mesh axis runs over, the one named last changes fastest.
Arguments:
- nodes: bfloat16 [4, 64, 32, 256], P('rep', 'graph'), may hold values from -20 to 20, as said below
- cotangent: bfloat16 [4, 64, 32, 256], P('rep', 'graph'), may hold values from -6 to 6
- live: int32 [4, 64], P('rep', 'graph'), may hold values from 2 to 32, as said below
- partner_first: int32 [4, 64], P('rep', 'graph'), may hold values from 0 to 63, as said below
- partner_size: int32 [4, 64], P('rep', 'graph'), may hold values from 1 to 2
- edge_src: int32 [4, 2048], P('rep', 'graph'), may hold values from 0 to 255, as said below
- edge_dst: int32 [4, 2048], P('rep', 'graph'), may hold values from 0 to 255, as said below
- w_edge1: bfloat16 [512, 512], replicated, may hold values from -0.25 to 0.25
- b_edge: float32 [512], replicated, may hold values from -3 to 3
- w_edge2: bfloat16 [512, 256], replicated, may hold values from -0.25 to 0.25
- w_node1: bfloat16 [768, 512], replicated, may hold values from -0.21875 to 0.21875
- b_node: float32 [512], replicated, may hold values from -3 to 3
- w_node2: bfloat16 [512, 256], replicated, may hold values from -0.25 to 0.25
Outputs:
- updated: bfloat16 [4, 64, 32, 256], P('rep', 'graph')
- d_nodes: bfloat16 [4, 64, 32, 256], P('rep', 'graph')
- g_edge1: float32 [512, 512], P('rep')
- g_bedge: float32 [512], P('rep')
- g_edge2: float32 [512, 256], P('rep')
- g_node1: float32 [768, 512], P('rep')
- g_bnode: float32 [512], P('rep')
- g_node2: float32 [512, 256], P('rep')
The draws below stay inside these ranges and needn't reach their ends.
Inputs may be any that keep to these rules, and one draw needn't show every extreme that they name: A graph is one or two consecutive granules of one device, and every granule of a graph but its last is full; rows beyond live are padding. `partner_first`: index within the replica of the first granule of the partner graph, the same for all granules of a graph; pairing is mutual. Graphs in the lower half of a device's 8 granules pair with graphs in the upper half of some device's granules; the upper-half graphs of one device have partners on distinct devices. Within a replica every half of every device holds the same number of two-granule graphs. `edge_src`: row index within the device (granule times 32 plus row); both ends of an edge are live rows of the same graph. `edge_dst`: as edge_src. `nodes`: padding rows are zero.
All inputs are finite; a program needn't handle non-finite values.
Results may differ from the reference program's by a relative error of at most 0.023.
Values may be sent and summed in bfloat16 or wider, within the bound.
A program may use at most 128 MiB of HBM per device.

```python
import jax
import jax.numpy as jnp
from jax import lax

H = 256
FM = 512
BLK = 32
GMAX = 2
NB = 8
E_DEV = 256
G_ALL = 64
N_GRAPH = 8
N_REP = 4


def inverse_order(ordering):
    return jnp.zeros(ordering.shape, jnp.int32).at[ordering].set(jnp.arange(ordering.shape[0], dtype=jnp.int32))


def device_orders(stream):
    streams = jax.random.split(stream, N_GRAPH)
    return jax.vmap(lambda single: inverse_order(jax.random.permutation(single, N_GRAPH).astype(jnp.int32)))(streams)


def pick(member, lookup):
    return jnp.sum(jnp.where(member, lookup, 0), axis=2).astype(jnp.int32)


def layout_one(replica_key):
    peer_count = N_GRAPH
    half_count = NB // 2
    streams = jax.random.split(jax.random.fold_in(replica_key, 17), 8)
    lowest = max(half_count - peer_count, 1)
    highest = half_count // 2
    double_count = jax.random.randint(streams[0], (), lowest, highest + 1)
    graph_count = half_count - double_count
    offsets = jnp.arange(peer_count, dtype=jnp.int32)
    first_order = inverse_order(jax.random.permutation(streams[1], peer_count).astype(jnp.int32))
    active = first_order < graph_count
    size_moving = jnp.where(active, jnp.where(first_order < double_count, 2, 1), 0).astype(jnp.int32)
    second_order = inverse_order(jax.random.permutation(streams[2], peer_count).astype(jnp.int32))
    rank_active = jnp.sum(active[None, :] & (second_order[None, :] < second_order[:, None]), axis=1)
    size_staying = jnp.where(active, jnp.where(rank_active < double_count, 2, 1), 0).astype(jnp.int32)
    sigma = jax.random.permutation(streams[3], peer_count).astype(jnp.int32)
    sigma_inverse = inverse_order(sigma)
    tau = jax.random.permutation(streams[4], peer_count).astype(jnp.int32)
    tau_inverse = inverse_order(tau)
    order_moving = device_orders(streams[5])
    order_staying = device_orders(streams[6])
    start_moving = jnp.sum(size_moving[None, None, :] * (order_moving[:, None, :] < order_moving[:, :, None]), axis=2).astype(jnp.int32)
    start_staying = jnp.sum(size_staying[None, None, :] * (order_staying[:, None, :] < order_staying[:, :, None]), axis=2).astype(jnp.int32)
    staying_device = sigma_inverse[(tau[:, None] + offsets[None, :]) % peer_count]
    moving_device = tau_inverse[(sigma[:, None] - offsets[None, :]) % peer_count]
    spots = jnp.arange(half_count, dtype=jnp.int32)
    member_staying = active[None, None, :] & (start_staying[:, None, :] <= spots[None, :, None]) & (spots[None, :, None] < start_staying[:, None, :] + size_staying[None, None, :])
    member_moving = active[None, None, :] & (start_moving[:, None, :] <= spots[None, :, None]) & (spots[None, :, None] < start_moving[:, None, :] + size_moving[None, None, :])
    offset_low = pick(member_staying, offsets[None, None, :])
    first_low = pick(member_staying, start_staying[:, None, :])
    size_low = pick(member_staying, size_staying[None, None, :])
    mate_low = jnp.take_along_axis(moving_device, offset_low, axis=1)
    partner_low = mate_low * NB + half_count + start_moving[mate_low, offset_low]
    mate_size_low = size_moving[offset_low]
    offset_high = pick(member_moving, offsets[None, None, :])
    first_high = pick(member_moving, start_moving[:, None, :]) + half_count
    size_high = pick(member_moving, size_moving[None, None, :])
    mate_high = jnp.take_along_axis(staying_device, offset_high, axis=1)
    partner_high = mate_high * NB + start_staying[mate_high, offset_high]
    mate_size_high = size_staying[offset_high]
    partner = jnp.concatenate([partner_low, partner_high], axis=1).astype(jnp.int32)
    partner_sizes = jnp.concatenate([mate_size_low, mate_size_high], axis=1).astype(jnp.int32)
    own_local = jnp.concatenate([first_low, first_high], axis=1)
    own_size = jnp.concatenate([size_low, size_high], axis=1)
    place_index = jnp.arange(NB, dtype=jnp.int32)[None, :] - own_local
    lowest_live = max(2, BLK // 4)
    live_counts = jax.random.randint(streams[7], (peer_count, NB), lowest_live, BLK + 1)
    live_counts = jnp.where((own_size == 2) & (place_index == 0), BLK, live_counts).astype(jnp.int32)
    own_first = (jnp.arange(peer_count, dtype=jnp.int32)[:, None] * NB + own_local).astype(jnp.int32)
    return (live_counts.reshape(-1), partner.reshape(-1), partner_sizes.reshape(-1), own_first.reshape(-1), own_size.reshape(-1).astype(jnp.int32))


def edges_one(replica_key):
    live_counts, partner, partner_sizes, own_first, own_size = layout_one(replica_key)
    streams = jax.random.split(jax.random.fold_in(replica_key, 29), 4)
    device_base = jnp.arange(N_GRAPH, dtype=jnp.int32)[:, None] * NB
    target_local = jax.random.randint(streams[0], (N_GRAPH, E_DEV), 0, NB)
    target_granule = device_base + target_local
    target_row = jax.random.randint(streams[1], (N_GRAPH, E_DEV), 0, live_counts[target_granule])
    source_granule = own_first[target_granule] + jax.random.randint(streams[2], (N_GRAPH, E_DEV), 0, own_size[target_granule])
    source_row = jax.random.randint(streams[3], (N_GRAPH, E_DEV), 0, live_counts[source_granule])
    source_local = (source_granule - device_base) * BLK + source_row
    target_flat = target_local * BLK + target_row
    return (source_local.reshape(-1).astype(jnp.int32), target_flat.reshape(-1).astype(jnp.int32))


def nodes_one(replica_key):
    live_counts, partner, partner_sizes, own_first, own_size = layout_one(replica_key)
    streams = jax.random.split(jax.random.fold_in(replica_key, 41), 1)
    granules = N_GRAPH * NB
    values = jnp.clip(jax.random.normal(streams[0], (granules, BLK, H), jnp.float32), -6.0, 6.0)
    row_live = jnp.arange(BLK, dtype=jnp.int32)[None, :] < live_counts[:, None]
    return jnp.where(row_live[:, :, None], values, 0.0)


def over_replicas(key, maker):
    return jax.vmap(lambda replica_index: maker(jax.random.fold_in(key, replica_index)))(jnp.arange(N_REP, dtype=jnp.int32))


def draw_nodes(key, part):
    return over_replicas(key, nodes_one).astype(jnp.bfloat16)


def draw_live(key, part):
    return over_replicas(key, lambda replica_key: layout_one(replica_key)[0])


def draw_partner_first(key, part):
    return over_replicas(key, lambda replica_key: layout_one(replica_key)[1])


def draw_partner_size(key, part):
    return over_replicas(key, lambda replica_key: layout_one(replica_key)[2])


def draw_edge_src(key, part):
    return over_replicas(key, lambda replica_key: edges_one(replica_key)[0])


def draw_edge_dst(key, part):
    return over_replicas(key, lambda replica_key: edges_one(replica_key)[1])


def level_of(rng, extent, cuts, smallest, high):
    def one(dim, blocks):
        draws = jax.random.uniform(jax.random.fold_in(jax.random.fold_in(rng, 6), dim), (blocks,), jnp.float32, smallest / len(cuts), high / len(cuts))
        return jnp.repeat(jnp.exp(draws), extent[dim] // blocks).reshape((-1,) + (1,) * (len(extent) - dim - 1))

    level = one(*cuts[0])
    for cut in cuts[1:]:
        level = level * one(*cut)
    return level


def centred(key, extent, deviation, bound, cuts=(), kind=jnp.bfloat16):
    result = jax.random.normal(key, extent, jnp.float32) * deviation
    if len(cuts) > 0:
        result = level_of(key, extent, cuts, -0.22, 0.18) * result
    return jnp.clip(result, min=-bound, max=bound).astype(kind)


def setup_inputs(seed: int = 0) -> dict:
    key_of = jax.random.split(jax.random.key(seed), 14)
    return {
        "nodes": draw_nodes(jax.random.fold_in(key_of[13], 71), 0),
        "cotangent": centred(key_of[1], (N_REP, G_ALL, BLK, H), 1.0, 6.0, ((0, 4), (1, 8))),
        "live": draw_live(jax.random.fold_in(key_of[13], 71), 0),
        "partner_first": draw_partner_first(jax.random.fold_in(key_of[13], 71), 0),
        "partner_size": draw_partner_size(jax.random.fold_in(key_of[13], 71), 0),
        "edge_src": draw_edge_src(jax.random.fold_in(key_of[13], 71), 0),
        "edge_dst": draw_edge_dst(jax.random.fold_in(key_of[13], 71), 0),
        "w_edge1": centred(key_of[7], (2 * H, FM), (2 * H) ** -0.5, 0.25),
        "b_edge": centred(key_of[8], (FM,), 0.5, 3.0, (), jnp.float32),
        "w_edge2": centred(key_of[9], (FM, H), FM ** -0.5, 0.25),
        "w_node1": centred(key_of[10], (3 * H, FM), (3 * H) ** -0.5, 0.21875),
        "b_node": centred(key_of[11], (FM,), 0.5, 3.0, (), jnp.float32),
        "w_node2": centred(key_of[12], (FM, H), FM ** -0.5, 0.25),
    }


def silu_slope(values):
    sigmoid_value = jax.nn.sigmoid(values)
    return sigmoid_value * (1.0 + values * (1.0 - sigmoid_value))


def attend(queries, key_rows, key_mask):
    scale_factor = queries.shape[-1] ** -0.5
    scores = jnp.einsum("gqh,gkh->gqk", queries.astype(jnp.float32), key_rows.astype(jnp.float32), precision=lax.Precision.HIGHEST) * scale_factor
    scores = jnp.where(key_mask[:, None, :], scores, -jnp.inf)
    highest = jnp.max(scores, axis=-1, keepdims=True)
    powers = jnp.exp(scores - highest)
    softmax_out = powers / jnp.sum(powers, axis=-1, keepdims=True)
    softmax_low = softmax_out.astype(jnp.bfloat16)
    context = jnp.einsum("gqk,gkh->gqh", softmax_low.astype(jnp.float32), key_rows.astype(jnp.float32), precision=lax.Precision.HIGHEST)
    moved_rows = (queries.astype(jnp.float32) - context).astype(jnp.bfloat16)
    return moved_rows, softmax_out, softmax_low


def attend_back(queries, key_rows, softmax_out, softmax_low, grad_moved):
    scale_factor = queries.shape[-1] ** -0.5
    negated = (-grad_moved).astype(jnp.float32)
    keys_wide = key_rows.astype(jnp.float32)
    grad_probs = jnp.einsum("gqh,gkh->gqk", negated, keys_wide, precision=lax.Precision.HIGHEST)
    grad_keys = jnp.einsum("gqk,gqh->gkh", softmax_low.astype(jnp.float32), negated, precision=lax.Precision.HIGHEST)
    inner_sum = jnp.sum(softmax_out * grad_probs, axis=-1, keepdims=True)
    grad_scores = (softmax_out * (grad_probs - inner_sum) * scale_factor).astype(jnp.bfloat16)
    scores_wide = grad_scores.astype(jnp.float32)
    grad_queries = jnp.einsum("gqk,gkh->gqh", scores_wide, keys_wide, precision=lax.Precision.HIGHEST) + grad_moved.astype(jnp.float32)
    grad_keys = grad_keys + jnp.einsum("gqk,gqh->gkh", scores_wide, queries.astype(jnp.float32), precision=lax.Precision.HIGHEST)
    return grad_queries, grad_keys


def replica(nodes, cotangent, live, partner_first, partner_size, edge_src, edge_dst, w_edge1, b_edge, w_edge2, w_node1, b_node, w_node2):
    granules, block_rows, state_width = nodes.shape
    node_rows = nodes.reshape(-1, state_width)
    total_rows = node_rows.shape[0]
    positions = jnp.arange(block_rows, dtype=jnp.int32)
    row_mask = (positions[None, :] < live[:, None]).reshape(-1, 1)
    offsets = (jnp.arange(edge_src.shape[0], dtype=jnp.int32) // E_DEV) * (NB * block_rows)
    sources = (edge_src + offsets).astype(jnp.int32)
    targets = (edge_dst + offsets).astype(jnp.int32)

    pre_target = (jnp.dot(node_rows, w_edge1[:state_width], preferred_element_type=jnp.float32) + b_edge).astype(jnp.bfloat16)
    pre_source = jnp.dot(node_rows, w_edge1[state_width:], preferred_element_type=jnp.float32).astype(jnp.bfloat16)
    summed = pre_target[targets].astype(jnp.float32) + pre_source[sources].astype(jnp.float32)
    gathered = jax.ops.segment_sum(jax.nn.silu(summed), targets, num_segments=total_rows).astype(jnp.bfloat16)
    message = jnp.dot(gathered, w_edge2, preferred_element_type=jnp.float32).astype(jnp.bfloat16)

    key_index = jnp.minimum(partner_first[:, None] + jnp.arange(GMAX, dtype=jnp.int32)[None, :], granules - 1).astype(jnp.int32)
    size_mask = jnp.arange(GMAX, dtype=jnp.int32)[None, :] < partner_size[:, None]
    key_mask = (size_mask[:, :, None] & (positions[None, None, :] < live[key_index][:, :, None])).reshape(granules, GMAX * block_rows)
    key_rows = nodes[key_index].reshape(granules, GMAX * block_rows, state_width)
    moved_rows, softmax_out, softmax_low = attend(nodes, key_rows, key_mask)
    moved_flat = moved_rows.reshape(-1, state_width)

    hidden_pre = (jnp.dot(node_rows, w_node1[:state_width], preferred_element_type=jnp.float32)
                  + jnp.dot(message, w_node1[state_width:2 * state_width], preferred_element_type=jnp.float32)
                  + jnp.dot(moved_flat, w_node1[2 * state_width:], preferred_element_type=jnp.float32) + b_node)
    active = jax.nn.silu(hidden_pre).astype(jnp.bfloat16)
    updated = jnp.where(row_mask, node_rows.astype(jnp.float32) + jnp.dot(active, w_node2, preferred_element_type=jnp.float32), 0.0).astype(jnp.bfloat16)

    grad_out = jnp.where(row_mask, cotangent.reshape(-1, state_width), jnp.zeros((), jnp.bfloat16)).astype(jnp.bfloat16)
    g_node2 = jnp.dot(active.T, grad_out, preferred_element_type=jnp.float32)
    grad_hidden = (jnp.dot(grad_out, w_node2.T, preferred_element_type=jnp.float32) * silu_slope(hidden_pre)).astype(jnp.bfloat16)
    g_node1 = jnp.concatenate([jnp.dot(node_rows.T, grad_hidden, preferred_element_type=jnp.float32),
                               jnp.dot(message.T, grad_hidden, preferred_element_type=jnp.float32),
                               jnp.dot(moved_flat.T, grad_hidden, preferred_element_type=jnp.float32)], axis=0)
    g_bnode = jnp.sum(grad_hidden.astype(jnp.float32), axis=0)
    grad_rows = grad_out.astype(jnp.float32) + jnp.dot(grad_hidden, w_node1[:state_width].T, preferred_element_type=jnp.float32)
    grad_message = jnp.dot(grad_hidden, w_node1[state_width:2 * state_width].T, preferred_element_type=jnp.float32).astype(jnp.bfloat16)
    grad_moved = jnp.dot(grad_hidden, w_node1[2 * state_width:].T, preferred_element_type=jnp.float32).astype(jnp.bfloat16)

    grad_queries, grad_keys = attend_back(nodes, key_rows, softmax_out, softmax_low, grad_moved.reshape(granules, block_rows, state_width))
    attention_grad = grad_queries.at[key_index.reshape(-1)].add(grad_keys.reshape(granules * GMAX, block_rows, state_width))

    g_edge2 = jnp.dot(gathered.T, grad_message, preferred_element_type=jnp.float32)
    grad_gathered = jnp.dot(grad_message, w_edge2.T, preferred_element_type=jnp.float32).astype(jnp.bfloat16)
    edge_grad = grad_gathered[targets].astype(jnp.float32) * silu_slope(summed)
    grad_target = jax.ops.segment_sum(edge_grad, targets, num_segments=total_rows).astype(jnp.bfloat16)
    grad_source = jax.ops.segment_sum(edge_grad, sources, num_segments=total_rows).astype(jnp.bfloat16)
    g_edge1 = jnp.concatenate([jnp.dot(node_rows.T, grad_target, preferred_element_type=jnp.float32),
                               jnp.dot(node_rows.T, grad_source, preferred_element_type=jnp.float32)], axis=0)
    g_bedge = jnp.sum(grad_target.astype(jnp.float32), axis=0)
    grad_rows = (grad_rows + attention_grad.reshape(-1, state_width)
                 + jnp.dot(grad_target, w_edge1[:state_width].T, preferred_element_type=jnp.float32)
                 + jnp.dot(grad_source, w_edge1[state_width:].T, preferred_element_type=jnp.float32))
    d_nodes = jnp.where(row_mask, grad_rows, 0.0).astype(jnp.bfloat16)
    return (updated.reshape(granules, block_rows, state_width), d_nodes.reshape(granules, block_rows, state_width),
            g_edge1, g_bedge, g_edge2, g_node1, g_bnode, g_node2)


def reference(nodes, cotangent, live, partner_first, partner_size, edge_src, edge_dst, w_edge1, b_edge, w_edge2, w_node1, b_node, w_node2):
    def one_replica(inputs):
        return replica(inputs[0], inputs[1], inputs[2], inputs[3], inputs[4], inputs[5], inputs[6],
                       w_edge1, b_edge, w_edge2, w_node1, b_node, w_node2)

    results = lax.map(one_replica, (nodes, cotangent, live, partner_first, partner_size, edge_src, edge_dst))
    scale_factor = (N_REP * N_GRAPH * NB * BLK) ** -0.5
    grads = tuple(jnp.sum(item, axis=0) * scale_factor for item in results[2:])
    return (results[0], results[1], grads[0], grads[1], grads[2], grads[3], grads[4], grads[5])
```

```python
import functools

import jax
import jax.numpy as jnp
from jax import lax
from jax.experimental import pallas as pl
from jax.experimental.pallas import tpu as pltpu
from jax.sharding import PartitionSpec as P

GMAX = 2
LANES = 128
F32 = jnp.float32
BF16 = jnp.bfloat16


def dot_nn(a, b):
    return lax.dot_general(a, b, (((1,), (0,)), ((), ())), preferred_element_type=F32)


def dot_nt(a, b):
    return lax.dot_general(a, b, (((1,), (1,)), ((), ())), preferred_element_type=F32)


def dot_tn(a, b):
    return lax.dot_general(a, b, (((0,), (0,)), ((), ())), preferred_element_type=F32)


def sigmoid(v):
    return 1.0 / (1.0 + jnp.exp(-v))


def silu_slope(v, s):
    return s * (1.0 + v * (1.0 - s))


def round_up(value, unit):
    return -(-value // unit) * unit


def send(src, dst, send_sem, recv_sem, graph, rep):
    return pltpu.make_async_remote_copy(
        src_ref=src,
        dst_ref=dst,
        send_sem=send_sem,
        recv_sem=recv_sem,
        device_id={"graph": graph, "rep": rep},
        device_id_type=pl.DeviceIdType.MESH,
    )


class Reduce:
    def __init__(self, n_graph, n_rep, me, rep, refs):
        self.n, self.r, self.me, self.rep = n_graph, n_rep, me, rep
        (self.full, self.r0, self.a, self.r1, self.b, self.r2, self.got,
         self.s0, self.s1, self.v1, self.s2, self.v2, self.s3, self.v3) = refs
        self.chips = n_graph // 2
        self.core = lax.rem(me, 2)
        self.chip = lax.div(me, 2)
        self.half = self.full.shape[1] // 2
        self.ch = self.full.shape[1] // n_graph
        self.sends = []

    def go(self, copy):
        copy.start()
        self.sends.append(copy)

    def rows(self, start, size):
        return pl.ds(pl.multiple_of(start, 16), size)

    def start_core(self):
        other = 1 - self.core
        self.c0 = send(self.full.at[:, self.rows(other * self.half, self.half), :], self.r0,
                       self.s0.at[0], self.s0.at[1], self.chip * 2 + other, self.rep)
        self.go(self.c0)

    def start_plane(self):
        self.c0.wait_recv()
        mine = self.full[:, self.rows(self.core * self.half, self.half), :].astype(F32)
        self.a[...] = (mine + self.r0[...].astype(F32)).astype(BF16)
        self.c1 = []
        for d in range(1, self.chips):
            q = lax.rem(self.chip + d, self.chips)
            copy = send(self.a.at[:, self.rows(q * self.ch, self.ch), :], self.r1.at[d],
                        self.s1.at[d], self.v1.at[d], q * 2 + self.core, self.rep)
            self.go(copy)
            self.c1.append(copy)

    def start_rep(self):
        total = self.a[:, self.rows(self.chip * self.ch, self.ch), :].astype(F32)
        for copy in self.c1:
            copy.wait_recv()
        for d in range(1, self.chips):
            total = total + self.r1[d].astype(F32)
        self.b[...] = total.astype(BF16)
        self.c2 = []
        for d in range(1, self.r):
            z = lax.rem(self.rep + d, self.r)
            copy = send(self.b.at[z], self.r2.at[d], self.s2.at[d], self.v2.at[d], self.me, z)
            self.go(copy)
            self.c2.append(copy)

    def start_gather(self):
        total = self.b[self.rep].astype(F32)
        for copy in self.c2:
            copy.wait_recv()
        for d in range(1, self.r):
            total = total + self.r2[d].astype(F32)
        place = self.core * self.chips + self.chip
        self.got[place] = total.astype(BF16)
        self.c3 = []
        for d in range(1, self.n):
            to = lax.rem(self.me + d, self.n)
            self.go(send(self.got.at[place], self.got.at[place], self.s3.at[d], self.v3.at[d], to, self.rep))
            src = lax.rem(self.me + self.n - d, self.n)
            src_place = lax.rem(src, 2) * self.chips + lax.div(src, 2)
            self.c3.append(send(self.got.at[src_place], self.got.at[src_place],
                                self.s3.at[d], self.v3.at[d], to, self.rep))

    def finish(self):
        for copy in self.c3:
            copy.wait_recv()
        return self.got[...].reshape(self.n * self.ch, LANES)

    def drain(self):
        for copy in self.sends:
            copy.wait_send()


def put_grad(full, offset, grad, n_rep):
    share = grad.shape[0] // n_rep
    panels = grad.shape[1] // LANES
    low = grad.astype(BF16)
    for j in range(panels):
        full[:, offset + j * share : offset + (j + 1) * share, :] = low[
            :, j * LANES : (j + 1) * LANES
        ].reshape(n_rep, share, LANES)
    return offset + panels * share


def put_bias(full, offset, bias, n_rep):
    share = bias.shape[1] // n_rep
    count = full.shape[1] - offset
    first = lax.broadcasted_iota(jnp.int32, (count, LANES), 0) == 0
    for r in range(n_rep):
        row = bias[:, r * share : (r + 1) * share]
        if share < LANES:
            row = jnp.concatenate([row, jnp.zeros((1, LANES - share), F32)], axis=1)
        full[r, offset:, :] = jnp.where(first, row, 0.0).astype(BF16)


def take_grad(flat, offset, out, scale):
    share = out.shape[0]
    panels = out.shape[1] // LANES
    for j in range(panels):
        out[:, j * LANES : (j + 1) * LANES] = (
            flat[offset + j * share : offset + (j + 1) * share].astype(F32) * scale
        )
    return offset + panels * share


def take_bias(flat, offset, out, scale):
    rows = flat[offset : offset + 16].astype(F32) * scale
    out[...] = rows[0:1, : out.shape[1]]


def kernel(
    n_graph, n_rep,
    nodes, cot, live, partner, src_ref, dst_ref, we1, be, we2, wn1, bn, wn2,
    updated_out, dnodes_out, oe1, obe, oe2, on1, obn, on2,
    outgoing, arrived, keygrad, backsend, back, inv,
    x_send, x_recv, b_send, b_recv,
    *group_refs,
):
    me = lax.axis_index("graph")
    rep = lax.axis_index("rep")
    G, B, H = nodes.shape
    R = G * B
    half = G // 2
    E = src_ref.shape[1]
    per = len(group_refs) // 2
    node_group = Reduce(n_graph, n_rep, me, rep, group_refs[:per])
    edge_group = Reduce(n_graph, n_rep, me, rep, group_refs[per:])

    barrier = pltpu.get_barrier_semaphore()
    for d in range(1, n_graph):
        pl.semaphore_signal(barrier, inc=1, device_id={"graph": lax.rem(me + d, n_graph), "rep": rep},
                            device_id_type=pl.DeviceIdType.MESH)
    for d in range(1, n_rep):
        pl.semaphore_signal(barrier, inc=1, device_id={"graph": me, "rep": lax.rem(rep + d, n_rep)},
                            device_id_type=pl.DeviceIdType.MESH)

    def build(p, carry):
        lane = lax.broadcasted_iota(jnp.int32, (16, H), 1)
        row = lax.broadcasted_iota(jnp.int32, (16, H), 0)
        tile = jnp.zeros((16, H), F32)
        for h in range(2):
            first = jnp.int32(0)
            count = jnp.int32(0)
            for g in reversed(range(h * half, (h + 1) * half)):
                hit = partner[0, g] // G == p
                first = jnp.where(hit, g, first)
                count = count + jnp.where(hit, 1, 0)
            second = jnp.minimum(first + 1, G - 1)
            live1 = jnp.where(count > 0, live[0, first], 0)
            live2 = jnp.where(count > 1, live[0, second], 0)
            inv[0, p * 2 + h] = first
            inv[1, p * 2 + h] = count
            outgoing[p, h * GMAX * B : h * GMAX * B + B, :] = nodes[first]
            outgoing[p, h * GMAX * B + B : (h + 1) * GMAX * B, :] = nodes[second]
            bound = jnp.where(lane < B, live1, B + live2)
            bound = jnp.where(row == h, bound, 0)
            tile = tile + jnp.where(lane < bound, 1.0, 0.0)
        outgoing[p, 2 * GMAX * B :, :] = tile.astype(BF16)
        return carry

    lax.fori_loop(0, n_graph, build, 0)
    pl.semaphore_wait(barrier, n_graph + n_rep - 2)

    sends = []

    def exchange(src, dst, s_sem, r_sem):
        waits = []
        for d in range(1, n_graph):
            to = lax.rem(me + d, n_graph)
            frm = lax.rem(me + n_graph - d, n_graph)
            copy = send(src.at[to], dst.at[me], s_sem.at[d], r_sem.at[d], to, rep)
            copy.start()
            sends.append(copy)
            waits.append(send(src.at[to], dst.at[frm], s_sem.at[d], r_sem.at[d], to, rep))
        return waits

    waits = exchange(outgoing, arrived, x_send, x_recv)
    arrived[me] = outgoing[me]

    rows = nodes[...].reshape(R, H)
    row_ids = lax.broadcasted_iota(jnp.int32, (R, E), 0)
    hot = jnp.concatenate(
        [
            jnp.where(row_ids == dst_ref[...], 1.0, 0.0).astype(BF16),
            jnp.where(row_ids == src_ref[...], 1.0, 0.0).astype(BF16),
        ],
        axis=0,
    )
    pre = jnp.concatenate(
        [
            (dot_nn(rows, we1[:H]) + be[...]).astype(BF16),
            dot_nn(rows, we1[H:]).astype(BF16),
        ],
        axis=0,
    )
    summed = dot_tn(hot, pre)
    edge_sig = sigmoid(summed)
    gathered = dot_nn(hot[:R], (summed * edge_sig).astype(BF16)).astype(BF16)
    message = dot_nn(gathered, we2[...]).astype(BF16)
    hidden_pre = dot_nn(rows, wn1[:H]) + dot_nn(message, wn1[H : 2 * H]) + bn[...]
    position = lax.broadcasted_iota(jnp.int32, (B, H), 0)
    mask = jnp.concatenate(
        [jnp.where(position < live[0, g], 1.0, 0.0) for g in range(G)], axis=0
    ) > 0.5
    grad_out = jnp.where(mask, cot[...].reshape(R, H).astype(F32), 0.0).astype(BF16)
    back_hidden = dot_nt(grad_out, wn2[...])

    for copy in waits:
        copy.wait_recv()
    scale = H ** (-0.5)

    def peer(g):
        return partner[0, g] // G

    def keys_of(g):
        off = GMAX * B if g < half else 0
        return arrived[peer(g), off : off + GMAX * B, :]

    def block(values, g):
        return values[g * B : (g + 1) * B]

    score_list, mask_list = [], []
    for g in range(G):
        h = 1 if g < half else 0
        score_list.append(dot_nt(block(rows, g), keys_of(g)))
        tail = arrived[peer(g), 2 * GMAX * B :, :].astype(F32)
        mask_list.append(jnp.broadcast_to(tail[h : h + 1, : GMAX * B], (B, GMAX * B)))
    scores = jnp.concatenate(score_list, axis=0) * scale
    scores = jnp.where(jnp.concatenate(mask_list, axis=0) > 0.5, scores, -jnp.inf)
    powers = jnp.exp(scores - jnp.max(scores, axis=-1, keepdims=True))
    probs = powers / jnp.sum(powers, axis=-1, keepdims=True)
    low = probs.astype(BF16)
    context = jnp.concatenate([dot_nn(block(low, g), keys_of(g)) for g in range(G)], axis=0)
    moved = (rows.astype(F32) - context).astype(BF16)

    hidden_pre = hidden_pre + dot_nn(moved, wn1[2 * H :])
    sig = sigmoid(hidden_pre)
    active = (hidden_pre * sig).astype(BF16)
    grad_hidden = (back_hidden * silu_slope(hidden_pre, sig)).astype(BF16)
    grad_moved = dot_nt(grad_hidden, wn1[2 * H :]).astype(BF16)

    negated = -grad_moved
    grad_probs = jnp.concatenate(
        [dot_nt(block(negated, g), keys_of(g)) for g in range(G)], axis=0
    )
    inner = jnp.sum(probs * grad_probs, axis=-1, keepdims=True)
    grad_scores = (probs * (grad_probs - inner) * scale).astype(BF16)
    for g in range(G):
        left = jnp.concatenate([block(low, g), block(grad_scores, g)], axis=0)
        right = jnp.concatenate([block(negated, g), block(rows, g)], axis=0)
        keygrad[g] = dot_tn(left, right)

    def build_back(p, carry):
        for h in range(2):
            first = inv[0, p * 2 + h]
            count = inv[1, p * 2 + h]
            one = jnp.where(count > 0, 1.0, 0.0)
            two = jnp.where(count > 1, 1.0, 0.0)
            total = keygrad[first] * one + keygrad[jnp.minimum(first + 1, G - 1)] * two
            backsend[p, (1 - h) * GMAX : (2 - h) * GMAX] = total.astype(BF16).reshape(GMAX, B, H)
        return carry

    lax.fori_loop(0, n_graph, build_back, 0)
    back_waits = exchange(backsend, back, b_send, b_recv)
    back[me] = backsend[me]

    full = node_group.full
    pieces = jnp.concatenate(
        [dot_tn(rows, grad_hidden), dot_tn(message, grad_hidden), dot_tn(moved, grad_hidden)], axis=0
    )
    at = put_grad(full, 0, pieces, n_rep)
    at = put_grad(full, at, dot_tn(active, grad_out), n_rep)
    put_bias(full, at, jnp.sum(grad_hidden.astype(F32), axis=0, keepdims=True), n_rep)
    node_group.start_core()

    grad_message = dot_nt(grad_hidden, wn1[H : 2 * H]).astype(BF16)
    grad_gathered = dot_nt(grad_message, we2[...]).astype(BF16)
    edge_grad = (dot_tn(hot[:R], grad_gathered) * silu_slope(summed, edge_sig)).astype(BF16)
    both = dot_nn(hot, edge_grad).astype(BF16)
    grad_target, grad_source = both[:R], both[R:]
    node_group.start_plane()

    full = edge_group.full
    pieces = jnp.concatenate([dot_tn(rows, grad_target), dot_tn(rows, grad_source)], axis=0)
    at = put_grad(full, 0, pieces, n_rep)
    at = put_grad(full, at, dot_tn(gathered, grad_message), n_rep)
    put_bias(full, at, jnp.sum(grad_target.astype(F32), axis=0, keepdims=True), n_rep)
    edge_group.start_core()

    updated = jnp.where(mask, rows.astype(F32) + dot_nn(active, wn2[...]), 0.0)
    updated_out[...] = updated.astype(BF16).reshape(G, B, H)
    total = grad_out.astype(F32) + grad_moved.astype(F32)
    total = total + dot_nt(grad_hidden, wn1[:H])
    total = total + dot_nt(grad_target, we1[:H]) + dot_nt(grad_source, we1[H:])
    total = total + jnp.concatenate(
        [dot_nn(block(grad_scores, g), keys_of(g)) for g in range(G)], axis=0
    )
    edge_group.start_plane()
    for copy in back_waits:
        copy.wait_recv()
    returned = []
    for g in range(G):
        h = 0 if g < half else 1
        same = partner[0, g] == partner[0, g - 1] if g > 0 else False
        place = jnp.where(same, 1, 0)
        returned.append(back[peer(g), h * GMAX + place])
    total = total + jnp.concatenate(returned, axis=0).astype(F32)
    dnodes_out[...] = jnp.where(mask, total, 0.0).astype(BF16).reshape(G, B, H)

    node_group.start_rep()
    edge_group.start_rep()
    node_group.start_gather()
    edge_group.start_gather()
    grad_scale = (n_graph * n_rep * R) ** (-0.5)
    flat = node_group.finish()
    at = take_grad(flat, 0, on1, grad_scale)
    at = take_grad(flat, at, on2, grad_scale)
    take_bias(flat, at, obn, grad_scale)
    flat = edge_group.finish()
    at = take_grad(flat, 0, oe1, grad_scale)
    at = take_grad(flat, at, oe2, grad_scale)
    take_bias(flat, at, obe, grad_scale)
    for copy in sends:
        copy.wait_send()
    node_group.drain()
    edge_group.drain()


def group_scratch(shapes, n_graph, n_rep):
    rows = sum(s[0] // n_rep * (s[1] // LANES) for s in shapes)
    rows = round_up(rows + 16, 16 * n_graph)
    half, ch, chips = rows // 2, rows // n_graph, n_graph // 2
    dma = pltpu.SemaphoreType.DMA
    return [
        pltpu.VMEM((n_rep, rows, LANES), BF16),
        pltpu.VMEM((n_rep, half, LANES), BF16),
        pltpu.VMEM((n_rep, half, LANES), BF16),
        pltpu.VMEM((chips, n_rep, ch, LANES), BF16),
        pltpu.VMEM((n_rep, ch, LANES), BF16),
        pltpu.VMEM((n_rep, ch, LANES), BF16),
        pltpu.VMEM((n_graph, ch, LANES), BF16),
        dma((2,)),
        dma((chips,)),
        dma((chips,)),
        dma((n_rep,)),
        dma((n_rep,)),
        dma((n_graph,)),
        dma((n_graph,)),
    ]


def on_device(
    n_graph, n_rep,
    nodes, cotangent, live, partner_first, partner_size, edge_src, edge_dst,
    w_edge1, b_edge, w_edge2, w_node1, b_node, w_node2,
):
    _, G, B, H = nodes.shape
    FM = w_edge1.shape[1]
    rows_x = 2 * GMAX * B
    dma = pltpu.SemaphoreType.DMA
    vmem = pl.BlockSpec(memory_space=pltpu.VMEM)
    smem = pl.BlockSpec(memory_space=pltpu.SMEM)
    sds = jax.ShapeDtypeStruct

    def share(shape):
        return sds((shape[0] // n_rep,) + tuple(shape[1:]), F32)

    outs = pl.pallas_call(
        functools.partial(kernel, n_graph, n_rep),
        out_shape=(
            sds((G, B, H), BF16),
            sds((G, B, H), BF16),
            share(w_edge1.shape),
            sds((1, FM // n_rep), F32),
            share(w_edge2.shape),
            share(w_node1.shape),
            sds((1, FM // n_rep), F32),
            share(w_node2.shape),
        ),
        in_specs=[vmem, vmem, smem, smem] + [vmem] * 8,
        out_specs=(vmem,) * 8,
        scratch_shapes=[
            pltpu.VMEM((n_graph, rows_x + 16, H), BF16),
            pltpu.VMEM((n_graph, rows_x + 16, H), BF16),
            pltpu.VMEM((G, GMAX * B, H), F32),
            pltpu.VMEM((n_graph, 2 * GMAX, B, H), BF16),
            pltpu.VMEM((n_graph, 2 * GMAX, B, H), BF16),
            pltpu.SMEM((2, 2 * n_graph), jnp.int32),
            dma((n_graph,)),
            dma((n_graph,)),
            dma((n_graph,)),
            dma((n_graph,)),
        ]
        + group_scratch([w_node1.shape, w_node2.shape], n_graph, n_rep)
        + group_scratch([w_edge1.shape, w_edge2.shape], n_graph, n_rep),
        compiler_params=pltpu.CompilerParams(
            collective_id=0, has_side_effects=True, vmem_limit_bytes=64 * 1000 * 1000
        ),
    )(
        nodes[0], cotangent[0], live, partner_first, edge_src, edge_dst,
        w_edge1, b_edge.reshape(1, FM), w_edge2, w_node1, b_node.reshape(1, FM), w_node2,
    )
    return (
        outs[0][None],
        outs[1][None],
        outs[2],
        outs[3].reshape(-1),
        outs[4],
        outs[5],
        outs[6].reshape(-1),
        outs[7],
    )


def solution(mesh):
    rows = P("rep", "graph", None, None)
    ints = P("rep", "graph")
    return jax.shard_map(
        functools.partial(on_device, mesh.shape["graph"], mesh.shape["rep"]),
        mesh=mesh,
        in_specs=(rows, rows, ints, ints, ints, ints, ints) + (P(),) * 6,
        out_specs=(
            rows,
            rows,
            P("rep", None),
            P("rep"),
            P("rep", None),
            P("rep", None),
            P("rep"),
            P("rep", None),
        ),
        check_vma=False,
    )
```
